32 devices in a mesh: twist: 4 (over y, x), walk: 8 (over z, core).
Axes of the slice: x: 2, y: 2, z: 4, core: 2. Of those that a mesh axis runs over, the one named last changes fastest.
Arguments:
- positions: float32 [2048, 3, 128], P(('twist', 'walk')), parts along dimension 0, may hold values from 0 to 25.1327
- inverse_slater: float32 [2048, 64, 128], P(('twist', 'walk')), parts along dimension 0, may hold values from -0.75 to 0.75
- orbitals: float32 [8, 64, 1536], P('twist'), parts along dimension 0, may hold values from -0.109375 to 0.109375
- twist_angle: float32 [12], P('twist'), parts along dimension 0, may hold values from -0.125 to 0.125
- trial_energy: float32 [4], P('twist'), parts along dimension 0, may hold values from 2 to 8
- multiplicity: int32 [2048], P(('twist', 'walk')), parts along dimension 0, may hold values from 1 to 3
- anchor_device: int32 [2048, 1], P(('twist', 'walk')), parts along dimension 0, may hold values from 0 to 7; in each aligned block of 64 rows (0 to 63, 64 to 127, ...) at most 16 rows name the same one
- anchor_slot: int32 [2048], P(('twist', 'walk')), parts along dimension 0, may hold values from 0 to 63
- live_count: int32 [32], P(('twist', 'walk')), parts along dimension 0, may hold values from 32 to 64, as said below
Outputs:
- new_inverse: float32 [2048, 64, 128], P(('twist', 'walk')), parts along dimension 0
- new_positions: float32 [2048, 3, 128], P(('twist', 'walk')), parts along dimension 0
- walker_scalars: float32 [2, 2048], P(None, ('twist', 'walk')), parts along dimension 1
- group_stats: float32 [8], P('twist'), parts along dimension 0
The draws below stay inside these ranges and needn't reach their ends.
There are 4 independent parts, one for each index of `twist`. The reference program is written for one: setup_inputs(seed, part) draws one part's arguments, and reference() takes and returns one part's arrays. A program takes and returns all parts, laid end to end along the dimension named above; each array names one. Nothing has to cross between parts.
Inputs may be any that keep to these rules, and one draw needn't show every extreme that they name: `anchor_device`: within each device's 64 slots (its aligned block) no source device is named more than 16 times; in every draw some device names one source exactly 16 times. Slots of device d below live_count[d] are live, the rest empty; in every draw some device has all 64 slots live.
All inputs are finite; a program needn't handle non-finite values.
Results may differ from the reference program's by a relative error of at most 0.0004.
Values sent between devices are 32-bit elements; how exact they have to be, the bound alone decides.
A program may use at most 64 MiB of HBM per device.

```python
import math
import jax
import jax.numpy as jnp
import numpy as np
from jax import lax

WALK_DEV = 64
NE = 128
NORB = 64
NG = 1536
WALKERS = 512
CAP = 16
N_WALK = 8


def draw_positions(key, part):
    box_side = 25.1327
    small_side = 12.0
    key_side, key_shift, key_cell = jax.random.split(jax.random.fold_in(key, 29), 3)
    log_side = jax.random.uniform(key_side, (WALKERS, 1, 1), jnp.float32, math.log(small_side), math.log(box_side))
    side = jnp.exp(log_side)
    corner = jax.random.uniform(key_shift, (WALKERS, 3, 1), jnp.float32, 0.0, 1.0)
    inside = jax.random.uniform(key_cell, (WALKERS, 3, NE), jnp.float32, 0.0, 1.0)
    placed = corner * (box_side - side) + side * inside
    return jnp.clip(placed, 0.0, box_side).astype(jnp.float32)


def draw_live_count(key, part):
    key_count, key_full = jax.random.split(jax.random.fold_in(key, 17))
    devices = WALKERS // WALK_DEV
    counts = jax.random.randint(key_count, (devices,), WALK_DEV // 2, WALK_DEV + 1)
    chosen = jax.random.randint(key_full, (), 0, devices)
    device_ids = jnp.arange(devices)
    lowest = (chosen + 1) % devices
    counts = jnp.where(device_ids == lowest, WALK_DEV // 2, counts)
    return jnp.where(device_ids == chosen, WALK_DEV, counts).astype(jnp.int32)


def with_ends(array, rng, least, largest):
    spot = [jax.random.randint(jax.random.fold_in(rng, axis), (), 0, length) for axis, length in enumerate(array.shape)]
    main_axis = array.shape.index(max(array.shape))
    beside = spot[:main_axis] + [(spot[main_axis] + 1) % array.shape[main_axis]] + spot[main_axis + 1:]
    return array.at[tuple(spot)].set(least).at[tuple(beside)].set(largest)


def steps_of(own_key, dims, cuts, least, high):
    factor_of, own = 1.0, jax.random.fold_in(own_key, 6)
    for dim, blocks in cuts:
        draws = jnp.exp(jax.random.uniform(jax.random.fold_in(own, dim), (blocks,), jnp.float32, least / len(cuts), high / len(cuts)))
        factor_of = factor_of * jnp.repeat(draws, dims[dim] // blocks).reshape([-1 if axis == dim else 1 for axis in range(len(dims))])
    return factor_of


def assign_block(rng, own, number, rows, amount, top, limit, lean):
    ranking = jax.random.permutation(rng, amount)
    crowded, ordinary = shares(amount, rows * top, limit, lean, True), shares(amount, rows * top, limit, lean, False)
    places = jnp.arange(amount)

    def named(sizes, offset_by):
        used = int((sizes > 0).sum())
        fixed = max(1, used // 4)
        passed = fixed + (places - fixed + offset_by * (used - fixed)) % max(1, amount - fixed)
        return jnp.zeros((amount,), jnp.int32).at[ranking[jnp.where(places < fixed, places, passed)]].set(jnp.asarray(sizes, jnp.int32))

    sizes = jnp.where(number % 4 == 0, named(crowded, number // 4), named(ordinary, number - number // 4 - 1))
    mixed = jax.random.permutation(jax.random.fold_in(own, 3), amount)
    giver, receiver = mixed[0:amount // 2 * 2:2], mixed[1:amount // 2 * 2:2]
    margin = jnp.minimum(sizes[giver] - 1, limit - sizes[receiver]) // 2
    margin = jnp.where((giver == ranking[0]) | (receiver == ranking[0]) | (sizes[receiver] == 0), 0, jnp.maximum(margin, 0))
    passed = jax.random.randint(jax.random.fold_in(own, 4), (amount // 2,), 0, 1 << 20) % (margin + 1)
    sizes = sizes.at[giver].add(-passed).at[receiver].add(passed)
    members = jnp.searchsorted(jnp.cumsum(sizes), jnp.arange(rows * top), side="right").astype(jnp.int32)
    table = members.reshape(top, rows).T
    table = table[jax.random.permutation(jax.random.fold_in(own, 1), rows)]
    offset_by = jax.random.randint(jax.random.fold_in(own, 2), (rows, 1), 0, top)
    return jnp.take_along_axis(table, (jnp.arange(top)[None, :] + offset_by) % top, axis=1)


def shares(count, total, reach, slope, full):
    portions = [(1 << 20) // math.isqrt(rank ** slope) + 1 for rank in range(1, count + 1)]
    largest = reach if full else min(reach, max(-(-total // count), total * portions[0] // sum(portions)))
    least = 1 if total - largest >= count - 1 else 0
    given, rest = [largest] + [least] * (count - 1), total - largest - least * (count - 1)
    while rest > 0:
        movable = [i for i in range(1, count) if given[i] < largest] or [i for i in range(1, count) if given[i] < reach]
        pool, budget = sum([portions[i] for i in movable]), rest
        for i in movable:
            extra = min(reach - given[i], max(1, budget * portions[i] // pool), rest)
            given[i] = given[i] + extra
            rest = rest - extra
    return np.array(given)


def noise(key, shape, spread, most, cuts=(), kind=jnp.bfloat16):
    factor_of = steps_of(key, shape, cuts, -0.22, 0.18) if cuts else 1.0
    values = jax.random.normal(key, shape, jnp.float32) * spread * factor_of
    return jnp.minimum(jnp.maximum(values, -most), most).astype(kind)


def setup_inputs(seed: int = 0, part: int = 0) -> dict:
    key_of = jax.random.split(jax.random.key(seed), 10)
    own_keys = jax.random.split(jax.random.fold_in(key_of[9], part), 10)
    positions = draw_positions(jax.random.fold_in(jax.random.fold_in(key_of[9], part), 71), part)
    inverse_slater = noise(own_keys[1], (WALKERS, NORB, NE), NORB ** -0.5, 0.75, ((0, 8),), jnp.float32)
    orbitals = noise(own_keys[2], (2, NORB, NG), (2 * NG) ** -0.5, 0.109375, (), jnp.float32)
    twist_angle = jnp.clip(jax.random.uniform(own_keys[3], (3,), jnp.float32, -0.125, 0.125), -0.125, 0.125)
    trial_energy = jnp.clip(jax.random.uniform(own_keys[4], (1,), jnp.float32, 2.0, 8.0), 2.0, 8.0)
    multiplicity = with_ends(jax.random.randint(own_keys[5], (WALKERS,), 1, 4), jax.random.fold_in(own_keys[5], 1), 1, 3).astype(jnp.int32)
    anchor_device_keys = jax.random.split(jax.random.fold_in(own_keys[6], 1), WALKERS // WALK_DEV)
    anchor_device_turns = jax.random.permutation(jax.random.fold_in(own_keys[6], 3), WALKERS // WALK_DEV)
    anchor_device = jax.vmap(lambda own, number: assign_block(jax.random.fold_in(own_keys[6], 2), own, number, WALK_DEV, N_WALK, 1, CAP, 2))(anchor_device_keys, anchor_device_turns).reshape((WALKERS, 1))
    anchor_slot = with_ends(jax.random.randint(own_keys[7], (WALKERS,), 0, WALK_DEV), jax.random.fold_in(own_keys[7], 1), 0, WALK_DEV - 1).astype(jnp.int32)
    live_count = draw_live_count(jax.random.fold_in(jax.random.fold_in(key_of[9], part), 71), part)
    return dict(positions=positions, inverse_slater=inverse_slater, orbitals=orbitals, twist_angle=twist_angle, trial_energy=trial_energy, multiplicity=multiplicity, anchor_device=anchor_device, anchor_slot=anchor_slot, live_count=live_count)


time_step = 0.1

def wave_momenta(twist_angle, plane_count):
    wave_index = jnp.arange(plane_count, dtype=jnp.int32)
    integer_grid = jnp.stack([wave_index // 64 - plane_count // 128, wave_index // 8 % 8 - 4, wave_index % 8 - 4], axis=1)
    return twist_angle[None, :] + 0.25 * integer_grid.astype(jnp.float32)

def build_table(orbitals, momenta):
    cosine_part = orbitals[0]
    sine_part = orbitals[1]
    square_norm = momenta[:, 0] * momenta[:, 0] + momenta[:, 1] * momenta[:, 1] + momenta[:, 2] * momenta[:, 2]
    pieces = [jnp.concatenate([cosine_part, sine_part], axis=1)]
    for axis_id in range(3):
        component = momenta[:, axis_id][None, :]
        pieces.append(jnp.concatenate([component * sine_part, -component * cosine_part], axis=1))
    pieces.append(jnp.concatenate([-square_norm[None, :] * cosine_part, -square_norm[None, :] * sine_part], axis=1))
    return jnp.concatenate(pieces, axis=0).astype(jnp.bfloat16)

def plane_basis(momenta, position_block):
    phase_angle = momenta[:, 0][None, :, None] * position_block[:, 0][:, None, :] + momenta[:, 1][None, :, None] * position_block[:, 1][:, None, :] + momenta[:, 2][None, :, None] * position_block[:, 2][:, None, :]
    return jnp.concatenate([jnp.cos(phase_angle), jnp.sin(phase_angle)], axis=1).astype(jnp.bfloat16)

def pair_terms(position_block):
    offset = position_block[:, :, :, None] - position_block[:, :, None, :]
    square = offset[:, 0] * offset[:, 0] + offset[:, 1] * offset[:, 1] + offset[:, 2] * offset[:, 2]
    electrons = position_block.shape[2]
    labels = jnp.arange(electrons, dtype=jnp.int32)
    off_diag = (labels[:, None] != labels[None, :]).astype(jnp.float32)
    reciprocal = 1.0 / (9.0 + square)
    pair_grad = 54.0 * reciprocal * reciprocal * off_diag
    jastrow_grad = lax.optimization_barrier(jnp.sum(pair_grad[:, None] * offset, axis=3))
    jastrow_lap = lax.optimization_barrier(jnp.sum(off_diag * (162.0 * reciprocal * reciprocal - 216.0 * square * reciprocal * reciprocal * reciprocal), axis=2))
    potential = 0.5 * lax.optimization_barrier(jnp.sum(off_diag / jnp.sqrt(1.0 + square), axis=(1, 2)))
    return (jastrow_grad, jastrow_lap, potential)

def walker_energy(values, inverse_block, position_block):
    walkers = inverse_block.shape[0]
    orbital_count = inverse_block.shape[1]
    electrons = inverse_block.shape[2]
    orbital = values[:, :orbital_count]
    gradients = values[:, orbital_count:4 * orbital_count].reshape(walkers, 3, orbital_count, electrons)
    laplacian = values[:, 4 * orbital_count:]
    det_ratio = lax.optimization_barrier(jnp.sum(orbital * inverse_block, axis=1))
    det_grad = lax.optimization_barrier(jnp.sum(gradients * inverse_block[:, None], axis=2))
    det_lap = lax.optimization_barrier(jnp.sum(laplacian * inverse_block, axis=1))
    jastrow_grad, jastrow_lap, potential = pair_terms(position_block)
    cross_term = det_grad[:, 0] * jastrow_grad[:, 0] + det_grad[:, 1] * jastrow_grad[:, 1] + det_grad[:, 2] * jastrow_grad[:, 2]
    jastrow_square = jastrow_grad[:, 0] * jastrow_grad[:, 0] + jastrow_grad[:, 1] * jastrow_grad[:, 1] + jastrow_grad[:, 2] * jastrow_grad[:, 2]
    kinetic = (det_ratio * det_lap + 2.0 * det_ratio * cross_term + det_ratio * det_ratio * (jastrow_square + jastrow_lap)) / (1.0 + det_ratio * det_ratio)
    return (potential - 0.5 * lax.optimization_barrier(jnp.sum(kinetic, axis=1))) / electrons

def block_energy(coef_table, momenta, inverse_block, position_block):
    basis_block = plane_basis(momenta, position_block)
    values = jnp.einsum('cg,bgk->bck', coef_table.astype(jnp.float32), basis_block.astype(jnp.float32), precision=lax.Precision.HIGHEST)
    return walker_energy(values, inverse_block, position_block)

def reference(positions, inverse_slater, orbitals, twist_angle, trial_energy, multiplicity, anchor_device, anchor_slot, live_count):
    walkers = positions.shape[0]
    orbital_count = inverse_slater.shape[1]
    electrons = inverse_slater.shape[2]
    momenta = wave_momenta(twist_angle, orbitals.shape[2])
    coef_table = build_table(orbitals, momenta)
    group = 8
    inverse_blocks = inverse_slater.reshape(walkers // group, group, orbital_count, electrons)
    position_blocks = positions.reshape(walkers // group, group, 3, electrons)
    energy = lax.map(lambda blocks: block_energy(coef_table, momenta, blocks[0], blocks[1]), (inverse_blocks, position_blocks)).reshape(walkers)
    weight = jnp.exp(-time_step * (energy - trial_energy[0]))
    scaled = multiplicity.astype(jnp.float32) * weight
    group_stats = jnp.stack([jnp.sum(scaled * energy), jnp.sum(scaled)]) / walkers
    per_device = walkers // live_count.shape[0]
    slot_ids = jnp.arange(walkers, dtype=jnp.int32)
    live_slot = slot_ids % per_device < live_count[slot_ids // per_device]
    source = (anchor_device[:, 0] * per_device + anchor_slot).astype(jnp.int32)
    new_inverse = jnp.where(live_slot[:, None, None], jnp.take(inverse_slater, source, axis=0), 0.0)
    new_positions = jnp.where(live_slot[:, None, None], jnp.take(positions, source, axis=0), 0.0)
    carried = jnp.take(jnp.stack([weight, energy]), source, axis=1)
    walker_scalars = jnp.where(live_slot[None, :], carried, 0.0)
    return (new_inverse, new_positions, walker_scalars, group_stats)
```

```python
import jax
import jax.numpy as jnp
import numpy as np
from jax import lax
from jax.experimental import pallas as pl
from jax.experimental.pallas import tpu as pltpu
from jax.sharding import PartitionSpec as P

time_step = 0.1
side = 8


def wave_momenta(twist_angle, plane_count):
    wave_index = jnp.arange(plane_count, dtype=jnp.int32)
    integer_grid = jnp.stack(
        [wave_index // 64 - plane_count // 128, wave_index // 8 % 8 - 4, wave_index % 8 - 4], axis=1
    )
    return twist_angle[None, :] + 0.25 * integer_grid.astype(jnp.float32)


def build_table(orbitals, momenta):
    cosine_part = orbitals[0]
    sine_part = orbitals[1]
    square_norm = (
        momenta[:, 0] * momenta[:, 0]
        + momenta[:, 1] * momenta[:, 1]
        + momenta[:, 2] * momenta[:, 2]
    )
    pieces = [jnp.concatenate([cosine_part, sine_part], axis=1)]
    for axis_id in range(3):
        component = momenta[:, axis_id][None, :]
        pieces.append(jnp.concatenate([component * sine_part, -component * cosine_part], axis=1))
    pieces.append(
        jnp.concatenate(
            [-square_norm[None, :] * cosine_part, -square_norm[None, :] * sine_part], axis=1
        )
    )
    return jnp.concatenate(pieces, axis=0).astype(jnp.bfloat16)


def axis_waves(momenta, coordinate):
    angle = momenta[None, :, None] * coordinate[:, None, :]
    return jnp.concatenate([jnp.cos(angle), jnp.sin(angle)], axis=1)


def energy_kernel(
    table_ref, inverse_ref, x_ref, yz_ref, pos_ref, column_ref, out_ref, basis, product, det, pair
):
    group, orbital_count, electrons = inverse_ref.shape
    depth = x_ref.shape[1] // 2
    area = side * side
    planes = depth * area
    for w in range(group):
        cols = slice(w * electrons, (w + 1) * electrons)
        cy, sy, cz, sz = [yz_ref[w, k * side : (k + 1) * side, :] for k in range(4)]

        def outer(a, b):
            return (a[:, None, :] * b[None, :, :]).reshape(area, electrons)

        cyz = outer(cy, cz) - outer(sy, sz)
        syz = outer(sy, cz) + outer(cy, sz)
        for g in range(depth):
            cx, sx = x_ref[w, g : g + 1, :], x_ref[w, depth + g : depth + g + 1, :]
            basis[g * area : (g + 1) * area, cols] = (cx * cyz - sx * syz).astype(jnp.bfloat16)
            basis[planes + g * area : planes + (g + 1) * area, cols] = (
                sx * cyz + cx * syz
            ).astype(jnp.bfloat16)
    product[...] = jnp.dot(table_ref[...], basis[...], preferred_element_type=jnp.float32)
    for w in range(group):
        cols = slice(w * electrons, (w + 1) * electrons)
        inverse = inverse_ref[w]
        for k in range(5):
            block = product[k * orbital_count : (k + 1) * orbital_count, cols]
            det[k, w : w + 1, :] = jnp.sum(block * inverse, axis=0, keepdims=True)
        chunk = 32
        sums = [jnp.zeros((chunk, electrons), jnp.float32) for _ in range(5)]
        here = [jnp.broadcast_to(pos_ref[w, a : a + 1, :], (chunk, electrons)) for a in range(3)]
        for first in range(0, electrons, chunk):
            offs = [
                here[a] - column_ref[w, first : first + chunk, a : a + 1] for a in range(3)
            ]
            square = offs[0] * offs[0] + offs[1] * offs[1] + offs[2] * offs[2]
            inv = 1.0 / (9.0 + square)
            inv2 = inv * inv
            for a in range(3):
                sums[a] = sums[a] + inv2 * offs[a]
            sums[3] = sums[3] + inv2 * (1944.0 * inv - 54.0)
            sums[4] = sums[4] + lax.rsqrt(1.0 + square)
        for k in range(5):
            pair[k, w : w + 1, :] = jnp.sum(sums[k], axis=0, keepdims=True)
    ratio, lap = det[0], det[4]
    jas = [54.0 * pair[a] for a in range(3)]
    cross = det[1] * jas[0] + det[2] * jas[1] + det[3] * jas[2]
    jas_square = jas[0] * jas[0] + jas[1] * jas[1] + jas[2] * jas[2]
    jas_lap = pair[3] - 2.0
    kinetic = (
        ratio * lap + 2.0 * ratio * cross + ratio * ratio * (jas_square + jas_lap)
    ) / (1.0 + ratio * ratio)
    out_ref[...] = 0.5 * ((pair[4] - 1.0) - kinetic)


def local_energies(table, momenta, inverse_slater, positions):
    walkers, orbital_count, electrons = inverse_slater.shape
    group = 8
    area = side * side
    planes = momenta.shape[0]
    x_rows = axis_waves(momenta[::area, 0], positions[:, 0])
    yz_rows = jnp.concatenate(
        [
            axis_waves(momenta[:area:side, 1], positions[:, 1]),
            axis_waves(momenta[:side, 2], positions[:, 2]),
        ],
        axis=1,
    )
    column = positions.transpose(0, 2, 1)

    def block(*shape):
        return pl.BlockSpec((group,) + shape, lambda i: (i,) + (0,) * len(shape))

    rows = pl.pallas_call(
        energy_kernel,
        out_shape=jax.ShapeDtypeStruct((walkers, electrons), jnp.float32),
        grid=(walkers // group,),
        in_specs=[
            pl.BlockSpec(table.shape, lambda i: (0, 0)),
            block(orbital_count, electrons),
            block(x_rows.shape[1], electrons),
            block(yz_rows.shape[1], electrons),
            block(3, electrons),
            block(electrons, 3),
        ],
        out_specs=block(electrons),
        scratch_shapes=[
            pltpu.VMEM((2 * planes, group * electrons), jnp.bfloat16),
            pltpu.VMEM((5 * orbital_count, group * electrons), jnp.float32),
            pltpu.VMEM((5, group, electrons), jnp.float32),
            pltpu.VMEM((5, group, electrons), jnp.float32),
        ],
        compiler_params=pltpu.CompilerParams(vmem_limit_bytes=40 * 1024 * 1024),
        cost_estimate=pl.CostEstimate(
            flops=2 * 5 * orbital_count * 2 * planes * walkers * electrons * 2,
            bytes_accessed=walkers * orbital_count * electrons * 4,
            transcendentals=walkers * electrons * electrons * 2,
        ),
    )(table, inverse_slater, x_rows, yz_rows, positions, column)
    return jnp.sum(rows, axis=1) / electrons


def build_requests(source_device, slot_rank, wanted, peer_count, capacity):
    peer_ids = jnp.arange(peer_count, dtype=jnp.int32)
    room_ids = jnp.arange(capacity, dtype=jnp.int32)
    matches = (source_device[None, None, :] == peer_ids[:, None, None]) & (
        slot_rank[None, None, :] == room_ids[None, :, None]
    )
    return jnp.sum(jnp.where(matches, wanted[None, None, :], 0), axis=2)


def body(
    positions,
    inverse_slater,
    orbitals,
    twist_angle,
    trial_energy,
    multiplicity,
    anchor_device,
    anchor_slot,
    live_count,
):
    walk_dev = positions.shape[0]
    orbital_count = inverse_slater.shape[1]
    electrons = inverse_slater.shape[2]
    peer_count = lax.axis_size("walk")
    capacity = min(walk_dev, max(2, 2 * walk_dev // peer_count))
    slot_ids = jnp.arange(walk_dev, dtype=jnp.int32)
    source_device = anchor_device[:, 0]
    same_source = (source_device[:, None] == source_device[None, :]) & (
        slot_ids[None, :] < slot_ids[:, None]
    )
    slot_rank = jnp.sum(same_source.astype(jnp.int32), axis=1)
    requests = build_requests(source_device, slot_rank, anchor_slot, peer_count, capacity)
    served = lax.all_to_all(requests, "walk", split_axis=0, concat_axis=0, tiled=True)
    served_flat = served.reshape(peer_count * capacity)
    send_inverse = jnp.take(inverse_slater, served_flat, axis=0).reshape(
        peer_count, capacity, orbital_count, electrons
    )
    send_positions = jnp.take(positions, served_flat, axis=0).reshape(
        peer_count, capacity, 3, electrons
    )
    recv_inverse, recv_positions = (
        lax.all_to_all(send_inverse, "walk", split_axis=0, concat_axis=0, tiled=True),
        lax.all_to_all(send_positions, "walk", split_axis=0, concat_axis=0, tiled=True),
    )
    momenta = wave_momenta(twist_angle, orbitals.shape[2])
    table = build_table(orbitals, momenta)
    energy = local_energies(table, momenta, inverse_slater, positions)
    weight = jnp.exp(-time_step * (energy - trial_energy[0]))
    scaled = multiplicity.astype(jnp.float32) * weight
    shared = lax.all_gather(jnp.stack([weight, energy, scaled]), "walk")
    group_stats = jnp.stack(
        [jnp.sum(shared[:, 2] * shared[:, 1]), jnp.sum(shared[:, 2])]
    ) / (walk_dev * peer_count)
    target = source_device * capacity + slot_rank
    live_slot = slot_ids < live_count[0]
    new_inverse = jnp.where(
        live_slot[:, None, None],
        jnp.take(
            recv_inverse.reshape(peer_count * capacity, orbital_count, electrons), target, axis=0
        ),
        0.0,
    )
    new_positions = jnp.where(
        live_slot[:, None, None],
        jnp.take(recv_positions.reshape(peer_count * capacity, 3, electrons), target, axis=0),
        0.0,
    )
    source = source_device * walk_dev + anchor_slot
    carried = jnp.take(
        shared[:, :2].transpose(1, 0, 2).reshape(2, peer_count * walk_dev), source, axis=1
    )
    walker_scalars = jnp.where(live_slot[None, :], carried, 0.0)
    return (new_inverse, new_positions, walker_scalars, group_stats)


def solution(mesh):
    in_specs = (
        P(("twist", "walk"), None, None),
        P(("twist", "walk"), None, None),
        P("twist", None, None),
        P("twist"),
        P("twist"),
        P(("twist", "walk")),
        P(("twist", "walk"), None),
        P(("twist", "walk")),
        P(("twist", "walk")),
    )
    out_specs = (
        P(("twist", "walk"), None, None),
        P(("twist", "walk"), None, None),
        P(None, ("twist", "walk")),
        P("twist"),
    )
    return jax.shard_map(body, mesh=mesh, in_specs=in_specs, out_specs=out_specs, check_vma=False)
```

```python
import jax
import jax.numpy as jnp
import numpy as np
from jax import lax
from jax.experimental import pallas as pl
from jax.experimental.pallas import tpu as pltpu
from jax.sharding import PartitionSpec as P

time_step = 0.1
side = 8


def wave_momenta(twist_angle, plane_count):
    wave_index = jnp.arange(plane_count, dtype=jnp.int32)
    integer_grid = jnp.stack(
        [wave_index // 64 - plane_count // 128, wave_index // 8 % 8 - 4, wave_index % 8 - 4], axis=1
    )
    return twist_angle[None, :] + 0.25 * integer_grid.astype(jnp.float32)


def build_table(orbitals, momenta):
    cosine_part = orbitals[0]
    sine_part = orbitals[1]
    square_norm = (
        momenta[:, 0] * momenta[:, 0]
        + momenta[:, 1] * momenta[:, 1]
        + momenta[:, 2] * momenta[:, 2]
    )
    pieces = [jnp.concatenate([cosine_part, sine_part], axis=1)]
    for axis_id in range(3):
        component = momenta[:, axis_id][None, :]
        pieces.append(jnp.concatenate([component * sine_part, -component * cosine_part], axis=1))
    pieces.append(
        jnp.concatenate(
            [-square_norm[None, :] * cosine_part, -square_norm[None, :] * sine_part], axis=1
        )
    )
    return jnp.concatenate(pieces, axis=0).astype(jnp.bfloat16)


def axis_waves(momenta, coordinate):
    angle = momenta[None, :, None] * coordinate[:, None, :]
    return jnp.concatenate([jnp.cos(angle), jnp.sin(angle)], axis=1)


def energy_kernel(
    table_ref, inverse_ref, x_ref, yz_ref, pos_ref, column_ref, out_ref, basis, product, det, pair
):
    group, orbital_count, electrons = inverse_ref.shape
    depth = x_ref.shape[1] // 2
    area = side * side
    planes = depth * area
    for w in range(group):
        cols = slice(w * electrons, (w + 1) * electrons)
        cy, sy, cz, sz = [yz_ref[w, k * side : (k + 1) * side, :] for k in range(4)]

        def outer(a, b):
            return (a[:, None, :] * b[None, :, :]).reshape(area, electrons)

        cyz = outer(cy, cz) - outer(sy, sz)
        syz = outer(sy, cz) + outer(cy, sz)
        for g in range(depth):
            cx, sx = x_ref[w, g : g + 1, :], x_ref[w, depth + g : depth + g + 1, :]
            basis[g * area : (g + 1) * area, cols] = (cx * cyz - sx * syz).astype(jnp.bfloat16)
            basis[planes + g * area : planes + (g + 1) * area, cols] = (
                sx * cyz + cx * syz
            ).astype(jnp.bfloat16)
    product[...] = jnp.dot(table_ref[...], basis[...], preferred_element_type=jnp.float32)
    for w in range(group):
        cols = slice(w * electrons, (w + 1) * electrons)
        inverse = inverse_ref[w]
        for k in range(5):
            block = product[k * orbital_count : (k + 1) * orbital_count, cols]
            det[k, w : w + 1, :] = jnp.sum(block * inverse, axis=0, keepdims=True)
        chunk = 32
        sums = [jnp.zeros((chunk, electrons), jnp.float32) for _ in range(5)]
        here = [jnp.broadcast_to(pos_ref[w, a : a + 1, :], (chunk, electrons)) for a in range(3)]
        for first in range(0, electrons, chunk):
            offs = [
                here[a] - column_ref[w, first : first + chunk, a : a + 1] for a in range(3)
            ]
            square = offs[0] * offs[0] + offs[1] * offs[1] + offs[2] * offs[2]
            inv = 1.0 / (9.0 + square)
            inv2 = inv * inv
            for a in range(3):
                sums[a] = sums[a] + inv2 * offs[a]
            sums[3] = sums[3] + inv2 * (1944.0 * inv - 54.0)
            sums[4] = sums[4] + lax.rsqrt(1.0 + square)
        for k in range(5):
            pair[k, w : w + 1, :] = jnp.sum(sums[k], axis=0, keepdims=True)
    ratio, lap = det[0], det[4]
    jas = [54.0 * pair[a] for a in range(3)]
    cross = det[1] * jas[0] + det[2] * jas[1] + det[3] * jas[2]
    jas_square = jas[0] * jas[0] + jas[1] * jas[1] + jas[2] * jas[2]
    jas_lap = pair[3] - 2.0
    kinetic = (
        ratio * lap + 2.0 * ratio * cross + ratio * ratio * (jas_square + jas_lap)
    ) / (1.0 + ratio * ratio)
    out_ref[...] = 0.5 * ((pair[4] - 1.0) - kinetic)


def local_energies(table, momenta, inverse_slater, positions):
    walkers, orbital_count, electrons = inverse_slater.shape
    group = 8
    area = side * side
    planes = momenta.shape[0]
    x_rows = axis_waves(momenta[::area, 0], positions[:, 0])
    yz_rows = jnp.concatenate(
        [
            axis_waves(momenta[:area:side, 1], positions[:, 1]),
            axis_waves(momenta[:side, 2], positions[:, 2]),
        ],
        axis=1,
    )
    column = positions.transpose(0, 2, 1)

    def block(*shape):
        return pl.BlockSpec((group,) + shape, lambda i: (i,) + (0,) * len(shape))

    rows = pl.pallas_call(
        energy_kernel,
        out_shape=jax.ShapeDtypeStruct((walkers, electrons), jnp.float32),
        grid=(walkers // group,),
        in_specs=[
            pl.BlockSpec(table.shape, lambda i: (0, 0)),
            block(orbital_count, electrons),
            block(x_rows.shape[1], electrons),
            block(yz_rows.shape[1], electrons),
            block(3, electrons),
            block(electrons, 3),
        ],
        out_specs=block(electrons),
        scratch_shapes=[
            pltpu.VMEM((2 * planes, group * electrons), jnp.bfloat16),
            pltpu.VMEM((5 * orbital_count, group * electrons), jnp.float32),
            pltpu.VMEM((5, group, electrons), jnp.float32),
            pltpu.VMEM((5, group, electrons), jnp.float32),
        ],
        compiler_params=pltpu.CompilerParams(vmem_limit_bytes=40 * 1024 * 1024),
        cost_estimate=pl.CostEstimate(
            flops=2 * 5 * orbital_count * 2 * planes * walkers * electrons * 2,
            bytes_accessed=walkers * orbital_count * electrons * 4,
            transcendentals=walkers * electrons * electrons * 2,
        ),
    )(table, inverse_slater, x_rows, yz_rows, positions, column)
    return jnp.sum(rows, axis=1) / electrons


def build_requests(source_device, slot_rank, wanted, peer_count, capacity):
    peer_ids = jnp.arange(peer_count, dtype=jnp.int32)
    room_ids = jnp.arange(capacity, dtype=jnp.int32)
    matches = (source_device[None, None, :] == peer_ids[:, None, None]) & (
        slot_rank[None, None, :] == room_ids[None, :, None]
    )
    return jnp.sum(jnp.where(matches, wanted[None, None, :], 0), axis=2)


def state_kernel(device_ref, rank_ref, live_ref, held_ref, out_ref, sem):
    slots, rows, _ = out_ref.shape

    def copy(slot):
        first = pl.multiple_of(rank_ref[slot] * rows, 8)
        return pltpu.make_async_copy(
            held_ref.at[device_ref[slot], pl.ds(first, rows)], out_ref.at[slot], sem.at[slot]
        )

    @pl.loop(0, slots)
    def _(slot):
        @pl.when(slot < live_ref[0])
        def _():
            copy(slot).start()

        @pl.when(slot >= live_ref[0])
        def _():
            out_ref[slot] = jnp.zeros(out_ref.shape[1:], out_ref.dtype)

    @pl.loop(0, slots)
    def _(slot):
        @pl.when(slot < live_ref[0])
        def _():
            copy(slot).wait()


def gather_states(received, device, rank, live_count, rows):
    slots, electrons = device.shape[0], received.shape[2]
    smem = pl.BlockSpec(memory_space=pltpu.SMEM)
    return pl.pallas_call(
        state_kernel,
        out_shape=jax.ShapeDtypeStruct((slots, rows, electrons), received.dtype),
        in_specs=[smem, smem, smem, pl.BlockSpec(memory_space=pl.ANY)],
        out_specs=pl.BlockSpec(memory_space=pltpu.VMEM),
        scratch_shapes=[pltpu.SemaphoreType.DMA((slots,))],
    )(device, rank, live_count, received)


def body(
    positions,
    inverse_slater,
    orbitals,
    twist_angle,
    trial_energy,
    multiplicity,
    anchor_device,
    anchor_slot,
    live_count,
):
    walk_dev = positions.shape[0]
    orbital_count = inverse_slater.shape[1]
    electrons = inverse_slater.shape[2]
    peer_count = lax.axis_size("walk")
    capacity = min(walk_dev, max(2, 2 * walk_dev // peer_count))
    slot_ids = jnp.arange(walk_dev, dtype=jnp.int32)
    source_device = anchor_device[:, 0]
    same_source = (source_device[:, None] == source_device[None, :]) & (
        slot_ids[None, :] < slot_ids[:, None]
    )
    slot_rank = jnp.sum(same_source.astype(jnp.int32), axis=1)
    requests = build_requests(source_device, slot_rank, anchor_slot, peer_count, capacity)
    served = lax.all_to_all(requests, "walk", split_axis=0, concat_axis=0, tiled=True)
    served_flat = served.reshape(peer_count * capacity)
    send_inverse = jnp.take(inverse_slater, served_flat, axis=0, mode="clip").reshape(
        peer_count, capacity * orbital_count, electrons
    )
    send_positions = jnp.take(positions, served_flat, axis=0, mode="clip").reshape(
        peer_count, capacity * 3, electrons
    )
    send = jnp.concatenate([send_inverse, send_positions], axis=1)
    received = lax.all_to_all(send, "walk", split_axis=0, concat_axis=0, tiled=True)
    local_positions, orbitals, twist_angle, send = lax.optimization_barrier(
        (positions, orbitals, twist_angle, send)
    )
    momenta = wave_momenta(twist_angle, orbitals.shape[2])
    table = build_table(orbitals, momenta)
    energy = local_energies(table, momenta, inverse_slater, local_positions)
    weight = jnp.exp(-time_step * (energy - trial_energy[0]))
    scaled = multiplicity.astype(jnp.float32) * weight
    shared = lax.all_gather(jnp.stack([weight, energy, scaled]), "walk")
    group_stats = jnp.stack(
        [jnp.sum(shared[:, 2] * shared[:, 1]), jnp.sum(shared[:, 2])]
    ) / (walk_dev * peer_count)
    live_slot = slot_ids < live_count[0]
    split = capacity * orbital_count
    tail = received[:, split:].reshape(peer_count * capacity, 3, electrons)
    new_inverse = gather_states(received, source_device, slot_rank, live_count, orbital_count)
    new_positions = jnp.where(
        live_slot[:, None, None],
        jnp.take(tail, source_device * capacity + slot_rank, axis=0, mode="clip"),
        0.0,
    )
    source = source_device * walk_dev + anchor_slot
    carried = jnp.take(
        shared[:, :2].transpose(1, 0, 2).reshape(2, peer_count * walk_dev), source, axis=1
    )
    walker_scalars = jnp.where(live_slot[None, :], carried, 0.0)
    return (new_inverse, new_positions, walker_scalars, group_stats)


def solution(mesh):
    in_specs = (
        P(("twist", "walk"), None, None),
        P(("twist", "walk"), None, None),
        P("twist", None, None),
        P("twist"),
        P("twist"),
        P(("twist", "walk")),
        P(("twist", "walk"), None),
        P(("twist", "walk")),
        P(("twist", "walk")),
    )
    out_specs = (
        P(("twist", "walk"), None, None),
        P(("twist", "walk"), None, None),
        P(None, ("twist", "walk")),
        P("twist"),
    )
    return jax.shard_map(body, mesh=mesh, in_specs=in_specs, out_specs=out_specs, check_vma=False)
```

```python
import jax
import jax.numpy as jnp
import numpy as np
from jax import lax
from jax.experimental import pallas as pl
from jax.experimental.pallas import tpu as pltpu
from jax.sharding import PartitionSpec as P

time_step = 0.1
side = 8


def wave_momenta(twist_angle, plane_count):
    wave_index = jnp.arange(plane_count, dtype=jnp.int32)
    integer_grid = jnp.stack(
        [wave_index // 64 - plane_count // 128, wave_index // 8 % 8 - 4, wave_index % 8 - 4], axis=1
    )
    return twist_angle[None, :] + 0.25 * integer_grid.astype(jnp.float32)


def build_table(orbitals, momenta):
    cosine_part = orbitals[0]
    sine_part = orbitals[1]
    square_norm = (
        momenta[:, 0] * momenta[:, 0]
        + momenta[:, 1] * momenta[:, 1]
        + momenta[:, 2] * momenta[:, 2]
    )
    pieces = [jnp.concatenate([cosine_part, sine_part], axis=1)]
    for axis_id in range(3):
        component = momenta[:, axis_id][None, :]
        pieces.append(jnp.concatenate([component * sine_part, -component * cosine_part], axis=1))
    pieces.append(
        jnp.concatenate(
            [-square_norm[None, :] * cosine_part, -square_norm[None, :] * sine_part], axis=1
        )
    )
    return jnp.concatenate(pieces, axis=0).astype(jnp.bfloat16)


def axis_waves(momenta, coordinate):
    angle = momenta[None, :, None] * coordinate[:, None, :]
    return jnp.concatenate([jnp.cos(angle), jnp.sin(angle)], axis=1)


def energy_kernel(
    table_ref, inverse_ref, x_ref, yz_ref, pos_ref, column_ref, out_ref, basis, product, det, pair
):
    group, orbital_count, electrons = inverse_ref.shape
    depth = x_ref.shape[1] // 2
    area = side * side
    planes = depth * area
    for w in range(group):
        cols = slice(w * electrons, (w + 1) * electrons)
        cy, sy, cz, sz = [yz_ref[w, k * side : (k + 1) * side, :] for k in range(4)]

        def outer(a, b):
            return (a[:, None, :] * b[None, :, :]).reshape(area, electrons)

        cyz = outer(cy, cz) - outer(sy, sz)
        syz = outer(sy, cz) + outer(cy, sz)
        for g in range(depth):
            cx, sx = x_ref[w, g : g + 1, :], x_ref[w, depth + g : depth + g + 1, :]
            basis[g * area : (g + 1) * area, cols] = (cx * cyz - sx * syz).astype(jnp.bfloat16)
            basis[planes + g * area : planes + (g + 1) * area, cols] = (
                sx * cyz + cx * syz
            ).astype(jnp.bfloat16)
    product[...] = jnp.dot(table_ref[...], basis[...], preferred_element_type=jnp.float32)
    for w in range(group):
        cols = slice(w * electrons, (w + 1) * electrons)
        inverse = inverse_ref[w]
        for k in range(5):
            block = product[k * orbital_count : (k + 1) * orbital_count, cols]
            det[k, w : w + 1, :] = jnp.sum(block * inverse, axis=0, keepdims=True)
        chunk = 32
        sums = [jnp.zeros((chunk, electrons), jnp.float32) for _ in range(5)]
        here = [jnp.broadcast_to(pos_ref[w, a : a + 1, :], (chunk, electrons)) for a in range(3)]
        for first in range(0, electrons, chunk):
            offs = [
                here[a] - column_ref[w, first : first + chunk, a : a + 1] for a in range(3)
            ]
            square = offs[0] * offs[0] + offs[1] * offs[1] + offs[2] * offs[2]
            inv = 1.0 / (9.0 + square)
            inv2 = inv * inv
            for a in range(3):
                sums[a] = sums[a] + inv2 * offs[a]
            sums[3] = sums[3] + inv2 * (1944.0 * inv - 54.0)
            sums[4] = sums[4] + lax.rsqrt(1.0 + square)
        for k in range(5):
            pair[k, w : w + 1, :] = jnp.sum(sums[k], axis=0, keepdims=True)
    ratio, lap = det[0], det[4]
    jas = [54.0 * pair[a] for a in range(3)]
    cross = det[1] * jas[0] + det[2] * jas[1] + det[3] * jas[2]
    jas_square = jas[0] * jas[0] + jas[1] * jas[1] + jas[2] * jas[2]
    jas_lap = pair[3] - 2.0
    kinetic = (
        ratio * lap + 2.0 * ratio * cross + ratio * ratio * (jas_square + jas_lap)
    ) / (1.0 + ratio * ratio)
    out_ref[...] = 0.5 * ((pair[4] - 1.0) - kinetic)


def local_energies(table, momenta, inverse_slater, positions):
    walkers, orbital_count, electrons = inverse_slater.shape
    group = 8
    area = side * side
    planes = momenta.shape[0]
    x_rows = axis_waves(momenta[::area, 0], positions[:, 0])
    yz_rows = jnp.concatenate(
        [
            axis_waves(momenta[:area:side, 1], positions[:, 1]),
            axis_waves(momenta[:side, 2], positions[:, 2]),
        ],
        axis=1,
    )
    column = positions.transpose(0, 2, 1)

    def block(*shape):
        return pl.BlockSpec((group,) + shape, lambda i: (i,) + (0,) * len(shape))

    rows = pl.pallas_call(
        energy_kernel,
        out_shape=jax.ShapeDtypeStruct((walkers, electrons), jnp.float32),
        grid=(walkers // group,),
        in_specs=[
            pl.BlockSpec(table.shape, lambda i: (0, 0)),
            block(orbital_count, electrons),
            block(x_rows.shape[1], electrons),
            block(yz_rows.shape[1], electrons),
            block(3, electrons),
            block(electrons, 3),
        ],
        out_specs=block(electrons),
        scratch_shapes=[
            pltpu.VMEM((2 * planes, group * electrons), jnp.bfloat16),
            pltpu.VMEM((5 * orbital_count, group * electrons), jnp.float32),
            pltpu.VMEM((5, group, electrons), jnp.float32),
            pltpu.VMEM((5, group, electrons), jnp.float32),
        ],
        compiler_params=pltpu.CompilerParams(vmem_limit_bytes=40 * 1024 * 1024),
        cost_estimate=pl.CostEstimate(
            flops=2 * 5 * orbital_count * 2 * planes * walkers * electrons * 2,
            bytes_accessed=walkers * orbital_count * electrons * 4,
            transcendentals=walkers * electrons * electrons * 2,
        ),
    )(table, inverse_slater, x_rows, yz_rows, positions, column)
    return jnp.sum(rows, axis=1) / electrons


def build_requests(source_device, slot_rank, wanted, peer_count, capacity):
    peer_ids = jnp.arange(peer_count, dtype=jnp.int32)
    room_ids = jnp.arange(capacity, dtype=jnp.int32)
    matches = (source_device[None, None, :] == peer_ids[:, None, None]) & (
        slot_rank[None, None, :] == room_ids[None, :, None]
    )
    return jnp.sum(jnp.where(matches, wanted[None, None, :], 0), axis=2)


def state_kernel(device_ref, rank_ref, live_ref, held_ref, out_ref, sem):
    slots, rows, _ = out_ref.shape

    def copy(slot):
        first = pl.multiple_of(rank_ref[slot] * rows, 8)
        return pltpu.make_async_copy(
            held_ref.at[device_ref[slot], pl.ds(first, rows)], out_ref.at[slot], sem.at[slot]
        )

    @pl.loop(0, slots)
    def _(slot):
        @pl.when(slot < live_ref[0])
        def _():
            copy(slot).start()

        @pl.when(slot >= live_ref[0])
        def _():
            out_ref[slot] = jnp.zeros(out_ref.shape[1:], out_ref.dtype)

    @pl.loop(0, slots)
    def _(slot):
        @pl.when(slot < live_ref[0])
        def _():
            copy(slot).wait()


def gather_states(received, device, rank, live_count, rows):
    slots, electrons = device.shape[0], received.shape[2]
    smem = pl.BlockSpec(memory_space=pltpu.SMEM)
    return pl.pallas_call(
        state_kernel,
        out_shape=jax.ShapeDtypeStruct((slots, rows, electrons), received.dtype),
        in_specs=[smem, smem, smem, pl.BlockSpec(memory_space=pl.ANY)],
        out_specs=pl.BlockSpec(memory_space=pltpu.VMEM),
        scratch_shapes=[pltpu.SemaphoreType.DMA((slots,))],
    )(device, rank, live_count, received)


def pack_kernel(capacity, served_ref, held_ref, tail_ref, out_ref, sem):
    peers = out_ref.shape[0]
    rows = held_ref.shape[1]

    def copy(peer, room):
        slot = peer * capacity + room
        first = pl.multiple_of(room * rows, 8)
        return pltpu.make_async_copy(
            held_ref.at[served_ref[slot]], out_ref.at[peer, pl.ds(first, rows)], sem.at[slot]
        )

    @pl.loop(0, peers)
    def _(peer):
        for room in range(capacity):
            copy(peer, room).start()

    out_ref[:, capacity * rows :, :] = tail_ref[...]

    @pl.loop(0, peers)
    def _(peer):
        for room in range(capacity):
            copy(peer, room).wait()


def pack_states(held, served, tail):
    peers, extra, electrons = tail.shape
    capacity = served.shape[0] // peers
    return pl.pallas_call(
        lambda *refs: pack_kernel(capacity, *refs),
        out_shape=jax.ShapeDtypeStruct(
            (peers, capacity * held.shape[1] + extra, electrons), held.dtype
        ),
        in_specs=[
            pl.BlockSpec(memory_space=pltpu.SMEM),
            pl.BlockSpec(memory_space=pl.ANY),
            pl.BlockSpec(memory_space=pltpu.VMEM),
        ],
        out_specs=pl.BlockSpec(memory_space=pltpu.VMEM),
        scratch_shapes=[pltpu.SemaphoreType.DMA((peers * capacity,))],
    )(served, held, tail)


def body(
    positions,
    inverse_slater,
    orbitals,
    twist_angle,
    trial_energy,
    multiplicity,
    anchor_device,
    anchor_slot,
    live_count,
):
    walk_dev = positions.shape[0]
    orbital_count = inverse_slater.shape[1]
    electrons = inverse_slater.shape[2]
    peer_count = lax.axis_size("walk")
    capacity = min(walk_dev, max(2, 2 * walk_dev // peer_count))
    slot_ids = jnp.arange(walk_dev, dtype=jnp.int32)
    source_device = anchor_device[:, 0]
    same_source = (source_device[:, None] == source_device[None, :]) & (
        slot_ids[None, :] < slot_ids[:, None]
    )
    slot_rank = jnp.sum(same_source.astype(jnp.int32), axis=1)
    requests = build_requests(source_device, slot_rank, anchor_slot, peer_count, capacity)
    served = lax.all_to_all(requests, "walk", split_axis=0, concat_axis=0, tiled=True)
    served_flat = served.reshape(peer_count * capacity)
    send_positions = jnp.take(positions, served_flat, axis=0, mode="clip").reshape(
        peer_count, capacity * 3, electrons
    )
    send = pack_states(inverse_slater, served_flat, send_positions)
    received = lax.all_to_all(send, "walk", split_axis=0, concat_axis=0, tiled=True)
    local_positions, orbitals, twist_angle, send = lax.optimization_barrier(
        (positions, orbitals, twist_angle, send)
    )
    momenta = wave_momenta(twist_angle, orbitals.shape[2])
    table = build_table(orbitals, momenta)
    energy = local_energies(table, momenta, inverse_slater, local_positions)
    weight = jnp.exp(-time_step * (energy - trial_energy[0]))
    scaled = multiplicity.astype(jnp.float32) * weight
    shared = lax.all_gather(jnp.stack([weight, energy, scaled]), "walk")
    group_stats = jnp.stack(
        [jnp.sum(shared[:, 2] * shared[:, 1]), jnp.sum(shared[:, 2])]
    ) / (walk_dev * peer_count)
    live_slot = slot_ids < live_count[0]
    split = capacity * orbital_count
    tail = received[:, split:].reshape(peer_count * capacity, 3, electrons)
    new_inverse = gather_states(received, source_device, slot_rank, live_count, orbital_count)
    new_positions = jnp.where(
        live_slot[:, None, None],
        jnp.take(tail, source_device * capacity + slot_rank, axis=0, mode="clip"),
        0.0,
    )
    source = source_device * walk_dev + anchor_slot
    carried = jnp.take(
        shared[:, :2].transpose(1, 0, 2).reshape(2, peer_count * walk_dev), source, axis=1
    )
    walker_scalars = jnp.where(live_slot[None, :], carried, 0.0)
    return (new_inverse, new_positions, walker_scalars, group_stats)


def solution(mesh):
    in_specs = (
        P(("twist", "walk"), None, None),
        P(("twist", "walk"), None, None),
        P("twist", None, None),
        P("twist"),
        P("twist"),
        P(("twist", "walk")),
        P(("twist", "walk"), None),
        P(("twist", "walk")),
        P(("twist", "walk")),
    )
    out_specs = (
        P(("twist", "walk"), None, None),
        P(("twist", "walk"), None, None),
        P(None, ("twist", "walk")),
        P("twist"),
    )
    return jax.shard_map(body, mesh=mesh, in_specs=in_specs, out_specs=out_specs, check_vma=False)
```
